32 devices in a mesh: vec: 16 (over z, y, x), ao: 2 (over core).
Axes of the slice: x: 2, y: 2, z: 4, core: 2. Of those that a mesh axis runs over, the one named last changes fastest.
Arguments:
- cholesky: float32 [16, 1200, 1200], P('vec', 'ao'), may hold values from -6 to 6
- coefficients: float32 [2, 720000], P('ao', 'vec'), may hold values from -0.1875 to 0.1875
Outputs:
- mo_vectors: float32 [16, 128, 1072], P(None, 'vec', 'ao')
The draws below stay inside these ranges and needn't reach their ends.
All inputs are finite; a program needn't handle non-finite values.
Results may differ from the reference program's by a relative error of at most 0.0001.
Values sent between devices are 32-bit elements; how exact they have to be, the bound alone decides.
A program may use at most 64 MiB of HBM per device.

```python
import jax
import jax.numpy as jnp
from jax import lax

NAO = 1200
NOCC = 128
NVIR = 1072
NMO = 1200
HALF_AO = 600
NVEC = 16
N_AO = 2


def steps_of(key, shape, split, low, top_value):
    level, own = 1.0, jax.random.fold_in(key, 6)
    for position, blocks in split:
        steps = jnp.exp(jax.random.uniform(jax.random.fold_in(own, position), (blocks,), jnp.float32, low / len(split), top_value / len(split)))
        level = level * jnp.repeat(steps, shape[position] // blocks).reshape([-1 if axis == position else 1 for axis in range(len(shape))])
    return level


def bell_draw(stream_key, extent, width, most, split=(), kind=jnp.bfloat16):
    entries = width * jax.random.normal(stream_key, extent, jnp.float32)
    if split:
        entries = entries * steps_of(stream_key, extent, split, -0.22, 0.18)
    return jnp.clip(entries, -most, most).astype(kind)


def setup_inputs(seed: int = 0) -> dict:
    streams_of = jax.random.split(jax.random.key(seed), 3)
    cholesky = bell_draw(streams_of[0], (NVEC, NAO, NAO), 1.0, 6.0, ((0, 16), (1, 2)), jnp.float32)
    coefficients = bell_draw(streams_of[1], (N_AO, HALF_AO * NMO), NAO ** -0.5, 0.1875, ((0, 2), (1, 16)), jnp.float32)
    return dict(cholesky=cholesky, coefficients=coefficients)


def reference(cholesky, coefficients):
    matrix = coefficients.reshape(NAO, NOCC + NVIR)
    occupied = matrix[:, :NOCC]
    virtual = matrix[:, NOCC:]

    def transform_one(vector):
        left_half = jnp.dot(occupied.T, vector, precision=lax.Precision.HIGHEST, preferred_element_type=jnp.float32)
        return jnp.dot(left_half, virtual, precision=lax.Precision.HIGHEST, preferred_element_type=jnp.float32)

    return lax.map(transform_one, cholesky)
```

```python
import functools

import jax
import jax.numpy as jnp
from jax import lax
from jax.experimental import pallas as pl
from jax.experimental.pallas import tpu as pltpu
from jax.sharding import PartitionSpec as P

NOCC = 128
LANES = 128
MESH = pl.DeviceIdType.MESH
F32 = jnp.float32


def up_to(size, step):
    return -(-size // step) * step


def simple_body(cholesky, coefficients):
    half_rows = cholesky.shape[1]
    own_flat = lax.all_gather(coefficients, "vec", axis=1, tiled=True)
    own_rows = own_flat.reshape(half_rows, own_flat.shape[1] // half_rows)
    occupied_own = own_rows[:, :NOCC]
    partial_x = jnp.einsum(
        "mi,pmn->pin",
        occupied_own,
        cholesky,
        precision=lax.Precision.HIGHEST,
        preferred_element_type=jnp.float32,
    )
    x_block = lax.psum_scatter(partial_x, "ao", scatter_dimension=2, tiled=True)
    virtual_own = own_rows[:, NOCC:]
    partial_y = jnp.einsum(
        "pin,na->pia",
        x_block,
        virtual_own,
        precision=lax.Precision.HIGHEST,
        preferred_element_type=jnp.float32,
    )
    summed = lax.psum_scatter(partial_y, "ao", scatter_dimension=2, tiled=True)
    owned = lax.all_to_all(summed, "vec", split_axis=1, concat_axis=0, tiled=True)
    return owned


def split(value):
    high = value.astype(jnp.bfloat16)
    return high, (value - high.astype(F32)).astype(jnp.bfloat16)


def product(left, right):
    (lh, ll), (rh, rl) = left, right
    dot = functools.partial(jnp.dot, preferred_element_type=F32)
    return dot(lh, rh) + (dot(lh, rl) + dot(ll, rh))


def kernel(
    n, starts, rows, occ_ref, vir_ref, l_ref, out_ref,
    occ_all, vir_all, l_buf, occ_dense, vir_dense, x_full, x_out, x_in, x_send, x_recv, y_full, y_out, y_in,
    l_sem, occ_ss, occ_rs, vir_ss, vir_rs, x_ss, x_rs, pair_ss, pair_rs,
):
    me, core = lax.axis_index("vec"), lax.axis_index("ao")
    nz = n // 4
    x, y, z = me % 2, (me // 2) % 2, me // 4
    xp, yp = me + 1 - 2 * x, me + 2 - 4 * y
    half = l_ref.shape[0]
    nao = l_ref.shape[1]

    l_copy = pltpu.make_async_copy(l_ref, l_buf, l_sem)
    l_copy.start()

    barrier = pltpu.get_barrier_semaphore()
    for d in range(1, n):
        pl.semaphore_signal(barrier, inc=1, device_id=((me + d) % n, core), device_id_type=MESH)
    pl.semaphore_signal(barrier, inc=1, device_id=(me, 1 - core), device_id_type=MESH)
    pl.semaphore_wait(barrier, n)

    def occ_copy(w, to):
        return pltpu.make_async_remote_copy(
            src_ref=occ_ref, dst_ref=occ_all.at[w], send_sem=occ_ss.at[to], recv_sem=occ_rs.at[w],
            device_id=(to, core), device_id_type=MESH)

    def vir_copy(w, way, to, src=None):
        return pltpu.make_async_remote_copy(
            src_ref=vir_all.at[w] if src is None else src, dst_ref=vir_all.at[w],
            send_sem=vir_ss.at[way, w], recv_sem=vir_rs.at[w], device_id=(to, core), device_id_type=MESH)

    def x_copy(w, to):
        return pltpu.make_async_remote_copy(
            src_ref=x_send.at[to], dst_ref=x_recv.at[w], send_sem=x_ss.at[to], recv_sem=x_rs.at[w],
            device_id=(to, core), device_id_type=MESH)

    def pair_copy(which, src, dst):
        return pltpu.make_async_remote_copy(
            src_ref=src, dst_ref=dst, send_sem=pair_ss.at[which], recv_sem=pair_rs.at[which],
            device_id=(me, 1 - core), device_id_type=MESH)

    for d in range(1, n):
        occ_copy(me, (me + d) % n).start()
    pl.when(z < nz - 1)(lambda: vir_copy(me, 2, me + 4, vir_ref).start())
    pl.when(z > 0)(lambda: vir_copy(me, 3, me - 4, vir_ref).start())
    vir_copy(me, 0, xp, vir_ref).start()
    vir_copy(me, 1, yp, vir_ref).start()

    def line(k):
        @pl.when(z >= k)
        def _():
            w = me - 4 * k
            vir_copy(w, 2, me).wait_recv()
            pl.when(z < nz - 1)(lambda: vir_copy(w, 2, me + 4).start())
            vir_copy(w, 0, xp).start()
            vir_copy(w, 1, yp).start()

        @pl.when(z + k < nz)
        def _():
            w = me + 4 * k
            vir_copy(w, 3, me).wait_recv()
            pl.when(z > 0)(lambda: vir_copy(w, 3, me - 4).start())
            vir_copy(w, 0, xp).start()
            vir_copy(w, 1, yp).start()

    def plane(k):
        def one(zz, shift):
            wx, wy = xp + 4 * shift, yp + 4 * shift
            vir_copy(wx, 0, me).wait_recv()
            pl.when(zz % 2 == 0)(lambda: vir_copy(wx, 1, yp).start())
            vir_copy(wy, 1, me).wait_recv()
            pl.when(zz % 2 == 1)(lambda: vir_copy(wy, 0, xp).start())

        if k == 0:
            one(z, 0)
        else:
            pl.when(z >= k)(lambda: one(z - k, -k))
            pl.when(z + k < nz)(lambda: one(z + k, k))

    occ_all[me] = occ_ref[...]
    vir_all[me] = vir_ref[...]
    occ_dense[...] = jnp.zeros_like(occ_dense)
    vir_dense[...] = jnp.zeros_like(vir_dense)
    x_full[...] = jnp.zeros_like(x_full)
    line(1)
    for d in range(1, n):
        occ_copy((me + d) % n, me).wait_recv()
    for w in range(n):
        occ_dense[starts[w]:starts[w] + rows, :] += occ_all[w, :rows, :]
    l_copy.wait()
    occ_t = occ_dense[...].T[:, :half]
    x_full[:, :nao] = product(split(occ_t), split(l_buf[...]))
    whole = x_full[...]
    low = whole[:, :x_out.shape[1]]
    high = pltpu.roll(whole, x_full.shape[1] - half, 1)[:, :x_out.shape[1]]
    first = core == 0
    x_out[...] = jnp.where(first, high, low)
    x_own = jnp.where(first, low, high)
    pair_copy(0, x_out, x_in).start()
    plane(0)
    if nz > 2:
        line(2)
    pair_copy(0, x_out, x_in).wait_recv()
    x_sum = x_own + x_in[...]
    x_send[...] = x_sum.reshape(x_send.shape)
    if nz > 1:
        plane(1)
    for d in range(1, n):
        x_copy(me, (me + d) % n).start()
    x_recv[me] = x_send[me]
    for k in range(2, nz):
        if k + 1 < nz:
            line(k + 1)
        plane(k)
    for zz in range(nz):
        wd = (1 - x) + 2 * (1 - y) + 4 * zz
        vir_copy(wd, 0, me).wait_recv()
    for d in range(1, n):
        x_copy((me + d) % n, me).wait_recv()
    for w in range(n):
        vir_dense[starts[w]:starts[w] + rows, :] += vir_all[w, :rows, :]
    y_full[...] = product(split(x_recv[...].reshape(x_sum.shape)), split(vir_dense[...]))
    whole_y = y_full[...]
    low_y = whole_y[:, :y_out.shape[1]]
    high_y = pltpu.roll(whole_y, y_full.shape[1] - out_ref.shape[2], 1)[:, :y_out.shape[1]]
    y_out[...] = jnp.where(first, high_y, low_y)
    y_own = jnp.where(first, low_y, high_y)
    pair_copy(1, y_out, y_in).start()

    for d in range(1, n):
        occ_copy(me, (me + d) % n).wait_send()
        x_copy(me, (me + d) % n).wait_send()
    for zz in range(nz):
        w = x + 2 * y + 4 * zz
        vir_copy(w, 0, xp).wait_send()
        vir_copy(w, 1, yp).wait_send()
        pl.when((z >= zz) & (z < nz - 1))(lambda w=w: vir_copy(w, 2, xp).wait_send())
        pl.when((z <= zz) & (z > 0))(lambda w=w: vir_copy(w, 3, xp).wait_send())
        if zz % 2 == 0:
            vir_copy(xp + 4 * (zz - z), 1, yp).wait_send()
        else:
            vir_copy(yp + 4 * (zz - z), 0, xp).wait_send()
    pair_copy(0, x_out, x_in).wait_send()
    pair_copy(1, y_out, y_in).wait()
    out_ref[...] = (y_own + y_in[...])[:, :out_ref.shape[2]].reshape(out_ref.shape)


def body(n, cholesky, coefficients):
    if cholesky.shape[0] != 1:
        return simple_body(cholesky, coefficients)
    half, nao = cholesky.shape[1:]
    per = coefficients.shape[1]
    nmo = per * n // half
    nvir = nmo - NOCC
    offsets = [w * per % nmo for w in range(n)]
    starts = tuple(w * per // nmo for w in range(n))
    rows = max(-(-(offset + per) // nmo) for offset in offsets)
    deep = up_to(rows, 8)
    me = lax.axis_index("vec")
    flat = coefficients[0]
    total = deep * nmo
    framed = jnp.zeros((total,), F32)
    for offset in sorted(set(offsets)):
        here = jnp.pad(flat, (offset, total - per - offset))
        framed = jnp.where(me * per % nmo == offset, here, framed)
    framed = framed.reshape(deep, nmo)
    occ = framed[:, :NOCC]
    wide = up_to(nvir, LANES)
    vir = jnp.pad(framed[:, NOCC:], ((0, 0), (0, wide - nvir)))
    tall = up_to(max(half, starts[-1] + rows), LANES)
    part = up_to(nvir // 2, LANES)
    iblock = NOCC // n
    dma = pltpu.SemaphoreType.DMA
    vmem = pl.BlockSpec(memory_space=pltpu.VMEM)
    return pl.pallas_call(
        functools.partial(kernel, n, starts, rows),
        out_shape=jax.ShapeDtypeStruct((n, iblock, nvir // 2), F32),
        in_specs=[vmem, vmem, pl.BlockSpec(memory_space=pl.ANY)],
        out_specs=vmem,
        scratch_shapes=[
            pltpu.VMEM((n, deep, NOCC), F32),
            pltpu.VMEM((n, deep, wide), F32),
            pltpu.VMEM((half, nao), F32),
            pltpu.VMEM((tall, NOCC), F32),
            pltpu.VMEM((tall, wide), F32),
            pltpu.VMEM((NOCC, up_to(nao, LANES)), F32),
            pltpu.VMEM((NOCC, tall), F32),
            pltpu.VMEM((NOCC, tall), F32),
            pltpu.VMEM((n, iblock, tall), F32),
            pltpu.VMEM((n, iblock, tall), F32),
            pltpu.VMEM((NOCC, wide), F32),
            pltpu.VMEM((NOCC, part), F32),
            pltpu.VMEM((NOCC, part), F32),
            dma, dma((n,)), dma((n,)), dma((4, n)), dma((n,)), dma((n,)), dma((n,)), dma((2,)), dma((2,)),
        ],
        compiler_params=pltpu.CompilerParams(
            collective_id=0, has_side_effects=True, vmem_limit_bytes=60 * 1024 * 1024),
        name="transform",
    )(occ, vir, cholesky[0])


def solution(mesh):
    n = mesh.shape["vec"]
    in_specs = (P("vec", "ao", None), P("ao", "vec"))
    out_specs = P(None, "vec", "ao")
    lines = n % 4 == 0 and mesh.shape["ao"] == 2 and NOCC % (8 * n) == 0
    step = functools.partial(body, n) if lines else simple_body
    return jax.shard_map(step, mesh=mesh, in_specs=in_specs, out_specs=out_specs, check_vma=False)
```

```python
import functools

import jax
import jax.numpy as jnp
from jax import lax
from jax.experimental import pallas as pl
from jax.experimental.pallas import tpu as pltpu
from jax.sharding import PartitionSpec as P

NOCC = 128
LANES = 128
MESH = pl.DeviceIdType.MESH
F32 = jnp.float32
STEP, TURN = 16, 0


def up_to(size, step):
    return -(-size // step) * step


def simple_body(cholesky, coefficients):
    half_rows = cholesky.shape[1]
    own_flat = lax.all_gather(coefficients, "vec", axis=1, tiled=True)
    own_rows = own_flat.reshape(half_rows, own_flat.shape[1] // half_rows)
    occupied_own = own_rows[:, :NOCC]
    partial_x = jnp.einsum(
        "mi,pmn->pin",
        occupied_own,
        cholesky,
        precision=lax.Precision.HIGHEST,
        preferred_element_type=jnp.float32,
    )
    x_block = lax.psum_scatter(partial_x, "ao", scatter_dimension=2, tiled=True)
    virtual_own = own_rows[:, NOCC:]
    partial_y = jnp.einsum(
        "pin,na->pia",
        x_block,
        virtual_own,
        precision=lax.Precision.HIGHEST,
        preferred_element_type=jnp.float32,
    )
    summed = lax.psum_scatter(partial_y, "ao", scatter_dimension=2, tiled=True)
    owned = lax.all_to_all(summed, "vec", split_axis=1, concat_axis=0, tiled=True)
    return owned


def split(value):
    high = value.astype(jnp.bfloat16)
    return high, (value - high.astype(F32)).astype(jnp.bfloat16)


def product(left, right):
    (lh, ll), (rh, rl) = left, right
    dot = functools.partial(jnp.dot, preferred_element_type=F32)
    return dot(lh, rh) + (dot(lh, rl) + dot(ll, rh))


def kernel(
    n, starts, rows, pieces, plan, own_ref, l_ref, out_ref,
    rows_all, l_buf, occ_dense, vir_dense, x_full, x_out, x_in, x_send, x_recv, y_full, y_out, y_in,
    l_sem, occ_ss, occ_rs, vir_ss, vir_rs, x_ss, x_rs, pair_ss, pair_rs,
):
    me, core = lax.axis_index("vec"), lax.axis_index("ao")
    nz = n // 4
    x, y, z = me % 2, (me // 2) % 2, me // 4
    xp, yp, diag = me + 1 - 2 * x, me + 2 - 4 * y, me + 3 - 2 * x - 4 * y
    half, nao = l_ref.shape
    wide = vir_dense.shape[1]

    l_copy = pltpu.make_async_copy(l_ref, l_buf, l_sem)
    l_copy.start()
    rows_all[me, :, :own_ref.shape[1]] = own_ref[...]

    barrier = pltpu.get_barrier_semaphore()
    for d in range(1, n):
        pl.semaphore_signal(barrier, inc=1, device_id=((me + d) % n, core), device_id_type=MESH)
    pl.semaphore_signal(barrier, inc=1, device_id=(me, 1 - core), device_id_type=MESH)
    pl.semaphore_wait(barrier, n)

    def occ_copy(w, to):
        part = rows_all.at[w, :, pl.ds(0, NOCC)]
        return pltpu.make_async_remote_copy(
            src_ref=part, dst_ref=part, send_sem=occ_ss.at[to], recv_sem=occ_rs.at[w],
            device_id=(to, core), device_id_type=MESH)

    def vir_copy(p, w, way, to):
        part = rows_all.at[w, pl.ds(pieces[p][0], pieces[p][1]), pl.ds(NOCC, wide)]
        return pltpu.make_async_remote_copy(
            src_ref=part, dst_ref=part, send_sem=vir_ss.at[p, way, w], recv_sem=vir_rs.at[p, w],
            device_id=(to, core), device_id_type=MESH)

    def x_copy(w, to):
        return pltpu.make_async_remote_copy(
            src_ref=x_send.at[to], dst_ref=x_recv.at[w], send_sem=x_ss.at[to], recv_sem=x_rs.at[w],
            device_id=(to, core), device_id_type=MESH)

    def pair_copy(which, src, dst):
        return pltpu.make_async_remote_copy(
            src_ref=src, dst_ref=dst, send_sem=pair_ss.at[which], recv_sem=pair_rs.at[which],
            device_id=(me, 1 - core), device_id_type=MESH)

    def along(p, w, up=True, down=True):
        if up:
            pl.when(z < nz - 1)(lambda: vir_copy(p, w, 2, me + 4).start())
        if down:
            pl.when(z > 0)(lambda: vir_copy(p, w, 3, me - 4).start())

    def send_own(p):
        along(p, me)
        vir_copy(p, me, 0, xp).start()
        vir_copy(p, me, 1, yp).start()

    def line(k, p):
        if k >= nz:
            return
        for up in (True, False):
            @pl.when(z >= k if up else z + k < nz)
            def _():
                w = me - 4 * k if up else me + 4 * k
                vir_copy(p, w, 2, me).wait_recv()
                along(p, w, up, not up)
                vir_copy(p, w, 0, xp).start()
                vir_copy(p, w, 1, yp).start()

    def plane(k, p):
        def one(shift):
            wx, wy = xp + 4 * shift, yp + 4 * shift
            even = (z + shift) % 2 == 0
            cross = k == 0 or not pieces[p][2]
            vir_copy(p, wx, 0, me).wait_recv()
            if cross:
                pl.when(even)(lambda: vir_copy(p, wx, 1, yp).start())
            vir_copy(p, wy, 1, me).wait_recv()
            if cross:
                pl.when(jnp.logical_not(even))(lambda: vir_copy(p, wy, 0, xp).start())

        if k == 0:
            one(0)
        elif k < nz:
            pl.when(z >= k)(lambda: one(-k))
            pl.when(z + k < nz)(lambda: one(k))

    def corner(k, p):
        def one(shift, up, down):
            vir_copy(p, diag + 4 * shift, 0, me).wait_recv()
            if pieces[p][2]:
                along(p, diag + 4 * shift, up, down)

        if k == 0:
            one(0, True, True)
        elif k < nz:
            pl.when(z >= k)(lambda: one(-k, True, False))
            pl.when(z + k < nz)(lambda: one(k, False, True))

    first = core == 0
    state = {}

    def occ_start():
        for d in range(1, n):
            occ_copy(me, (me + d) % n).start()
        occ_dense[...] = jnp.zeros_like(occ_dense)
        vir_dense[...] = jnp.zeros_like(vir_dense)
        x_full[...] = jnp.zeros_like(x_full)

    def half_transform():
        for d in range(1, n):
            occ_copy((me + d) % n, me).wait_recv()
        for w in range(n):
            occ_dense[starts[w]:starts[w] + rows, :] += rows_all[w, :rows, :NOCC]
        l_copy.wait()
        occ_t = occ_dense[...].T[:, :half]
        x_full[:, :nao] = product(split(occ_t), split(l_buf[...]))
        whole = x_full[...]
        low = whole[:, :x_out.shape[1]]
        high = pltpu.roll(whole, x_full.shape[1] - half, 1)[:, :x_out.shape[1]]
        x_out[...] = jnp.where(first, high, low)
        state["own"] = jnp.where(first, low, high)
        pair_copy(0, x_out, x_in).start()

    def x_join():
        pair_copy(0, x_out, x_in).wait_recv()
        x_send[...] = (state["own"] + x_in[...]).reshape(x_send.shape)

    def x_start():
        for d in range(1, n):
            x_copy(me, (me + d) % n).start()
        x_recv[me] = x_send[me]

    def x_wait():
        for d in range(1, n):
            x_copy((me + d) % n, me).wait_recv()

    def join(w):
        vir_dense[starts[w]:starts[w] + rows, :] += rows_all[w, :rows, NOCC:]

    steps = dict(
        occ=occ_start, own=send_own, line=line, plane=plane, corner=corner,
        half=half_transform, xjoin=x_join, xstart=x_start, xwait=x_wait)
    for step, *args in plan:
        steps[step](*args)

    for w in range(n):
        join(w)
    y_full[...] = product(split(x_recv[...].reshape(x_out.shape)), split(vir_dense[...]))
    whole_y = y_full[...]
    low_y = whole_y[:, :y_out.shape[1]]
    high_y = pltpu.roll(whole_y, y_full.shape[1] - out_ref.shape[2], 1)[:, :y_out.shape[1]]
    y_out[...] = jnp.where(first, high_y, low_y)
    y_own = jnp.where(first, low_y, high_y)
    pair_copy(1, y_out, y_in).start()

    for d in range(1, n):
        occ_copy(me, (me + d) % n).wait_send()
        x_copy(me, (me + d) % n).wait_send()
    for p in range(len(pieces)):
        for zz in range(nz):
            w, wd = x + 2 * y + 4 * zz, diag + 4 * (zz - z)
            vir_copy(p, w, 0, xp).wait_send()
            vir_copy(p, w, 1, yp).wait_send()
            for slot in (w, wd) if pieces[p][2] else (w,):
                pl.when((z >= zz) & (z < nz - 1))(lambda: vir_copy(p, slot, 2, xp).wait_send())
                pl.when((z <= zz) & (z > 0))(lambda: vir_copy(p, slot, 3, xp).wait_send())
            crossed = (z == zz) if pieces[p][2] else (z >= 0)
            if zz % 2 == 0:
                pl.when(crossed)(lambda: vir_copy(p, xp + 4 * (zz - z), 1, yp).wait_send())
            else:
                pl.when(crossed)(lambda: vir_copy(p, yp + 4 * (zz - z), 0, xp).wait_send())
    pair_copy(0, x_out, x_in).wait_send()
    pair_copy(1, y_out, y_in).wait()
    out_ref[...] = (y_own + y_in[...])[:, :out_ref.shape[2]].reshape(out_ref.shape)


def plan_of(count, nz):
    every = range(count)
    plan = [("occ",)]
    plan += [("own", p) for p in every]
    plan += [("line", 1, p) for p in every]
    plan += [("half",)]
    plan += [("plane", 0, p) for p in every]
    plan += [("line", 2, p) for p in every]
    plan += [("xjoin",)]
    plan += [("plane", 1, p) for p in every]
    plan += [("xstart",)]
    plan += [("corner", 0, p) for p in every]
    for k in range(2, nz):
        plan += [("line", k + 1, p) for p in every]
        plan += [("plane", k, p) for p in every]
        plan += [("corner", k - 1, p) for p in every]
    plan += [("corner", nz - 1, p) for p in every]
    return plan + [("xwait",)]


def body(n, cholesky, coefficients):
    if cholesky.shape[0] != 1:
        return simple_body(cholesky, coefficients)
    half, nao = cholesky.shape[1:]
    per = coefficients.shape[1]
    nmo = per * n // half
    nvir = nmo - NOCC
    offsets = [w * per % nmo for w in range(n)]
    starts = tuple(w * per // nmo for w in range(n))
    rows = max(-(-(offset + per) // nmo) for offset in offsets)
    deep = up_to(rows, 8)
    me = lax.axis_index("vec")
    flat = coefficients[0]
    total = deep * nmo
    framed = jnp.zeros((total,), F32)
    for offset in sorted(set(offsets)):
        here = jnp.pad(flat, (offset, total - per - offset))
        framed = jnp.where(me * per % nmo == offset, here, framed)
    framed = framed.reshape(deep, nmo)
    wide = up_to(nvir, LANES)
    pieces = tuple((row, min(STEP, deep - row), row < TURN) for row in range(0, deep, STEP))
    plan = plan_of(len(pieces), n // 4)
    tall = up_to(max(half, starts[-1] + rows), LANES)
    part = up_to(nvir // 2, LANES)
    iblock = NOCC // n
    dma = pltpu.SemaphoreType.DMA
    vmem = pl.BlockSpec(memory_space=pltpu.VMEM)
    return pl.pallas_call(
        functools.partial(kernel, n, starts, rows, pieces, plan),
        out_shape=jax.ShapeDtypeStruct((n, iblock, nvir // 2), F32),
        in_specs=[vmem, pl.BlockSpec(memory_space=pl.ANY)],
        out_specs=vmem,
        scratch_shapes=[
            pltpu.VMEM((n, deep, NOCC + wide), F32),
            pltpu.VMEM((half, nao), F32),
            pltpu.VMEM((tall, NOCC), F32),
            pltpu.VMEM((tall, wide), F32),
            pltpu.VMEM((NOCC, up_to(nao, LANES)), F32),
            pltpu.VMEM((NOCC, tall), F32),
            pltpu.VMEM((NOCC, tall), F32),
            pltpu.VMEM((n, iblock, tall), F32),
            pltpu.VMEM((n, iblock, tall), F32),
            pltpu.VMEM((NOCC, wide), F32),
            pltpu.VMEM((NOCC, part), F32),
            pltpu.VMEM((NOCC, part), F32),
            dma, dma((n,)), dma((n,)), dma((len(pieces), 4, n)), dma((len(pieces), n)), dma((n,)), dma((n,)), dma((2,)), dma((2,)),
        ],
        compiler_params=pltpu.CompilerParams(
            collective_id=0, has_side_effects=True, vmem_limit_bytes=60 * 1024 * 1024),
        name="transform",
    )(framed, cholesky[0])


def solution(mesh):
    n = mesh.shape["vec"]
    in_specs = (P("vec", "ao", None), P("ao", "vec"))
    out_specs = P(None, "vec", "ao")
    lines = n % 4 == 0 and mesh.shape["ao"] == 2 and NOCC % (8 * n) == 0
    step = functools.partial(body, n) if lines else simple_body
    return jax.shard_map(step, mesh=mesh, in_specs=in_specs, out_specs=out_specs, check_vma=False)
```

```python
import functools

import jax
import jax.numpy as jnp
from jax import lax
from jax.experimental import pallas as pl
from jax.experimental.pallas import tpu as pltpu
from jax.sharding import PartitionSpec as P

NOCC = 128
LANES = 128
MESH = pl.DeviceIdType.MESH
F32 = jnp.float32
STEP, TURN = 24, 0


def up_to(size, step):
    return -(-size // step) * step


def simple_body(cholesky, coefficients):
    half_rows = cholesky.shape[1]
    own_flat = lax.all_gather(coefficients, "vec", axis=1, tiled=True)
    own_rows = own_flat.reshape(half_rows, own_flat.shape[1] // half_rows)
    occupied_own = own_rows[:, :NOCC]
    partial_x = jnp.einsum(
        "mi,pmn->pin",
        occupied_own,
        cholesky,
        precision=lax.Precision.HIGHEST,
        preferred_element_type=jnp.float32,
    )
    x_block = lax.psum_scatter(partial_x, "ao", scatter_dimension=2, tiled=True)
    virtual_own = own_rows[:, NOCC:]
    partial_y = jnp.einsum(
        "pin,na->pia",
        x_block,
        virtual_own,
        precision=lax.Precision.HIGHEST,
        preferred_element_type=jnp.float32,
    )
    summed = lax.psum_scatter(partial_y, "ao", scatter_dimension=2, tiled=True)
    owned = lax.all_to_all(summed, "vec", split_axis=1, concat_axis=0, tiled=True)
    return owned


def split(value):
    high = value.astype(jnp.bfloat16)
    return high, (value - high.astype(F32)).astype(jnp.bfloat16)


def product(left, right):
    (lh, ll), (rh, rl) = left, right
    dot = functools.partial(jnp.dot, preferred_element_type=F32)
    return dot(lh, rh) + (dot(lh, rl) + dot(ll, rh))


def kernel(
    n, starts, rows, pieces, plan, own_ref, l_ref, out_ref,
    rows_all, l_buf, occ_dense, vir_dense, x_full, x_out, x_in, x_send, x_recv, y_full, y_out, y_in,
    l_sem, occ_ss, occ_rs, vir_ss, vir_rs, x_ss, x_rs, pair_ss, pair_rs,
):
    me, core = lax.axis_index("vec"), lax.axis_index("ao")
    nz = n // 4
    x, y, z = me % 2, (me // 2) % 2, me // 4
    xp, yp, diag = me + 1 - 2 * x, me + 2 - 4 * y, me + 3 - 2 * x - 4 * y
    half, nao = l_ref.shape
    wide = vir_dense.shape[1]

    l_copy = pltpu.make_async_copy(l_ref, l_buf, l_sem)
    l_copy.start()
    rows_all[me, :, :own_ref.shape[1]] = own_ref[...]

    barrier = pltpu.get_barrier_semaphore()
    for d in range(1, n):
        pl.semaphore_signal(barrier, inc=1, device_id=((me + d) % n, core), device_id_type=MESH)
    pl.semaphore_signal(barrier, inc=1, device_id=(me, 1 - core), device_id_type=MESH)
    pl.semaphore_wait(barrier, n)

    def occ_copy(w, way, to):
        part = rows_all.at[w, :, pl.ds(0, NOCC)]
        return pltpu.make_async_remote_copy(
            src_ref=part, dst_ref=part, send_sem=occ_ss.at[way, to if way == 3 else w], recv_sem=occ_rs.at[w],
            device_id=(to, core), device_id_type=MESH)

    def vir_copy(p, w, way, to):
        part = rows_all.at[w, pl.ds(pieces[p][0], pieces[p][1]), pl.ds(NOCC, wide)]
        return pltpu.make_async_remote_copy(
            src_ref=part, dst_ref=part, send_sem=vir_ss.at[p, way, w], recv_sem=vir_rs.at[p, w],
            device_id=(to, core), device_id_type=MESH)

    def x_copy(w, to):
        return pltpu.make_async_remote_copy(
            src_ref=x_send.at[to], dst_ref=x_recv.at[w], send_sem=x_ss.at[to], recv_sem=x_rs.at[w],
            device_id=(to, core), device_id_type=MESH)

    def pair_copy(which, src, dst):
        return pltpu.make_async_remote_copy(
            src_ref=src, dst_ref=dst, send_sem=pair_ss.at[which], recv_sem=pair_rs.at[which],
            device_id=(me, 1 - core), device_id_type=MESH)

    def along(p, w, up=True, down=True):
        if up:
            pl.when(z < nz - 1)(lambda: vir_copy(p, w, 2, me + 4).start())
        if down:
            pl.when(z > 0)(lambda: vir_copy(p, w, 3, me - 4).start())

    def send_own(p):
        along(p, me)
        vir_copy(p, me, 0, xp).start()
        vir_copy(p, me, 1, yp).start()

    def line(k, p):
        if k >= nz:
            return
        for up in (True, False):
            @pl.when(z >= k if up else z + k < nz)
            def _():
                w = me - 4 * k if up else me + 4 * k
                vir_copy(p, w, 2, me).wait_recv()
                along(p, w, up, not up)
                vir_copy(p, w, 0, xp).start()
                vir_copy(p, w, 1, yp).start()

    def plane(k, p):
        def one(shift):
            wx, wy = xp + 4 * shift, yp + 4 * shift
            even = (z + shift) % 2 == 0
            cross = k == 0 or not pieces[p][2]
            vir_copy(p, wx, 0, me).wait_recv()
            if cross:
                pl.when(even)(lambda: vir_copy(p, wx, 1, yp).start())
            vir_copy(p, wy, 1, me).wait_recv()
            if cross:
                pl.when(jnp.logical_not(even))(lambda: vir_copy(p, wy, 0, xp).start())

        if k == 0:
            one(0)
        elif k < nz:
            pl.when(z >= k)(lambda: one(-k))
            pl.when(z + k < nz)(lambda: one(k))

    def corner(k, p):
        def one(shift, up, down):
            vir_copy(p, diag + 4 * shift, 0, me).wait_recv()
            if pieces[p][2]:
                along(p, diag + 4 * shift, up, down)

        if k == 0:
            one(0, True, True)
        elif k < nz:
            pl.when(z >= k)(lambda: one(-k, True, False))
            pl.when(z + k < nz)(lambda: one(k, False, True))

    first = core == 0
    state = {}

    def occ_spread(w):
        for way, to in enumerate((xp, yp, diag)):
            occ_copy(w, way, to).start()

    def occ_line():
        for d in range(1, nz):
            w = (me + 4 * d) % n
            occ_copy(w, 3, me).wait_recv()
            occ_spread(w)

    def occ_start():
        for d in range(1, nz):
            occ_copy(me, 3, (me + 4 * d) % n).start()
        occ_spread(me)
        occ_dense[...] = jnp.zeros_like(occ_dense)
        vir_dense[...] = jnp.zeros_like(vir_dense)
        x_full[...] = jnp.zeros_like(x_full)

    def half_transform():
        for d in range(nz):
            for other in (xp, yp, diag):
                occ_copy((other + 4 * d) % n, 3, me).wait_recv()
        for w in range(n):
            occ_dense[starts[w]:starts[w] + rows, :] += rows_all[w, :rows, :NOCC]
        l_copy.wait()
        occ_t = occ_dense[...].T[:, :half]
        x_full[:, :nao] = product(split(occ_t), split(l_buf[...]))
        whole = x_full[...]
        low = whole[:, :x_out.shape[1]]
        high = pltpu.roll(whole, x_full.shape[1] - half, 1)[:, :x_out.shape[1]]
        x_out[...] = jnp.where(first, high, low)
        state["own"] = jnp.where(first, low, high)
        pair_copy(0, x_out, x_in).start()

    def x_join():
        pair_copy(0, x_out, x_in).wait_recv()
        x_send[...] = (state["own"] + x_in[...]).reshape(x_send.shape)

    def x_start():
        for d in range(1, n):
            x_copy(me, (me + d) % n).start()
        x_recv[me] = x_send[me]

    def x_wait():
        for d in range(1, n):
            x_copy((me + d) % n, me).wait_recv()

    def join(w):
        vir_dense[starts[w]:starts[w] + rows, :] += rows_all[w, :rows, NOCC:]

    steps = dict(
        occ=occ_start, occline=occ_line, own=send_own, line=line, plane=plane, corner=corner,
        half=half_transform, xjoin=x_join, xstart=x_start, xwait=x_wait)
    for step, *args in plan:
        steps[step](*args)

    for w in range(n):
        join(w)
    y_full[...] = product(split(x_recv[...].reshape(x_out.shape)), split(vir_dense[...]))
    whole_y = y_full[...]
    low_y = whole_y[:, :y_out.shape[1]]
    high_y = pltpu.roll(whole_y, y_full.shape[1] - out_ref.shape[2], 1)[:, :y_out.shape[1]]
    y_out[...] = jnp.where(first, high_y, low_y)
    y_own = jnp.where(first, low_y, high_y)
    pair_copy(1, y_out, y_in).start()

    for d in range(1, n):
        x_copy(me, (me + d) % n).wait_send()
    for d in range(nz):
        for way in range(3):
            occ_copy((me + 4 * d) % n, way, xp).wait_send()
        if d:
            occ_copy(me, 3, (me + 4 * d) % n).wait_send()
    for p in range(len(pieces)):
        for zz in range(nz):
            w, wd = x + 2 * y + 4 * zz, diag + 4 * (zz - z)
            vir_copy(p, w, 0, xp).wait_send()
            vir_copy(p, w, 1, yp).wait_send()
            for slot in (w, wd) if pieces[p][2] else (w,):
                pl.when((z >= zz) & (z < nz - 1))(lambda: vir_copy(p, slot, 2, xp).wait_send())
                pl.when((z <= zz) & (z > 0))(lambda: vir_copy(p, slot, 3, xp).wait_send())
            crossed = (z == zz) if pieces[p][2] else (z >= 0)
            if zz % 2 == 0:
                pl.when(crossed)(lambda: vir_copy(p, xp + 4 * (zz - z), 1, yp).wait_send())
            else:
                pl.when(crossed)(lambda: vir_copy(p, yp + 4 * (zz - z), 0, xp).wait_send())
    pair_copy(0, x_out, x_in).wait_send()
    pair_copy(1, y_out, y_in).wait()
    out_ref[...] = (y_own + y_in[...])[:, :out_ref.shape[2]].reshape(out_ref.shape)


def plan_of(count, nz):
    every = range(count)

    def wave(name, k):
        return [(name, k, p) for p in every]

    plan = [("occ",), ("own", 0), ("occline",)] + [("own", p) for p in every[1:]]
    plan += wave("line", 1) + wave("plane", 0) + wave("line", 2) + [("half",)] + wave("plane", 1) + [("xjoin",)] + wave("line", 3) + [("xstart",)] + wave("corner", 0)
    plan += wave("plane", 2) + wave("corner", 1)
    for k in range(3, nz):
        plan += wave("line", k + 1) + wave("plane", k) + wave("corner", k - 1)
    return plan + wave("corner", nz - 1) + [("xwait",)]


def body(n, cholesky, coefficients):
    if cholesky.shape[0] != 1:
        return simple_body(cholesky, coefficients)
    half, nao = cholesky.shape[1:]
    per = coefficients.shape[1]
    nmo = per * n // half
    nvir = nmo - NOCC
    offsets = [w * per % nmo for w in range(n)]
    starts = tuple(w * per // nmo for w in range(n))
    rows = max(-(-(offset + per) // nmo) for offset in offsets)
    deep = up_to(rows, 8)
    me = lax.axis_index("vec")
    flat = coefficients[0]
    total = deep * nmo
    framed = jnp.zeros((total,), F32)
    for offset in sorted(set(offsets)):
        here = jnp.pad(flat, (offset, total - per - offset))
        framed = jnp.where(me * per % nmo == offset, here, framed)
    framed = framed.reshape(deep, nmo)
    wide = up_to(nvir, LANES)
    pieces = tuple((row, min(STEP, deep - row), row < TURN) for row in range(0, deep, STEP))
    plan = plan_of(len(pieces), n // 4)
    tall = up_to(max(half, starts[-1] + rows), LANES)
    part = up_to(nvir // 2, LANES)
    iblock = NOCC // n
    dma = pltpu.SemaphoreType.DMA
    vmem = pl.BlockSpec(memory_space=pltpu.VMEM)
    return pl.pallas_call(
        functools.partial(kernel, n, starts, rows, pieces, plan),
        out_shape=jax.ShapeDtypeStruct((n, iblock, nvir // 2), F32),
        in_specs=[vmem, pl.BlockSpec(memory_space=pl.ANY)],
        out_specs=vmem,
        scratch_shapes=[
            pltpu.VMEM((n, deep, NOCC + wide), F32),
            pltpu.VMEM((half, nao), F32),
            pltpu.VMEM((tall, NOCC), F32),
            pltpu.VMEM((tall, wide), F32),
            pltpu.VMEM((NOCC, up_to(nao, LANES)), F32),
            pltpu.VMEM((NOCC, tall), F32),
            pltpu.VMEM((NOCC, tall), F32),
            pltpu.VMEM((n, iblock, tall), F32),
            pltpu.VMEM((n, iblock, tall), F32),
            pltpu.VMEM((NOCC, wide), F32),
            pltpu.VMEM((NOCC, part), F32),
            pltpu.VMEM((NOCC, part), F32),
            dma, dma((4, n)), dma((n,)), dma((len(pieces), 4, n)), dma((len(pieces), n)), dma((n,)), dma((n,)), dma((2,)), dma((2,)),
        ],
        compiler_params=pltpu.CompilerParams(
            collective_id=0, has_side_effects=True, vmem_limit_bytes=60 * 1024 * 1024),
        name="transform",
    )(framed, cholesky[0])


def solution(mesh):
    n = mesh.shape["vec"]
    in_specs = (P("vec", "ao", None), P("ao", "vec"))
    out_specs = P(None, "vec", "ao")
    lines = n % 4 == 0 and mesh.shape["ao"] == 2 and NOCC % (8 * n) == 0
    step = functools.partial(body, n) if lines else simple_body
    return jax.shard_map(step, mesh=mesh, in_specs=in_specs, out_specs=out_specs, check_vma=False)
```
